32 devices in a mesh: grp: 8 (over z, x), vocab: 4 (over y, core).
Axes of the slice: x: 2, y: 2, z: 4, core: 2. Of those that a mesh axis runs over, the one named last changes fastest.
Arguments:
- teacher_rows: bfloat16 [64, 8, 4096], P('grp', None, 'vocab'), may hold values from -160 to 160
- student_rows: bfloat16 [8, 32, 5120], P('grp', None, 'vocab'), may hold values from -160 to 160
- teacher_head: bfloat16 [4096, 8192], P(None, ('grp', 'vocab')), may hold values from -0.25 to 0.25
- student_head: bfloat16 [5120, 8192], P(None, ('grp', 'vocab')), may hold values from -0.25 to 0.25
- lengths: int32 [64], replicated, may hold values from 1 to 8, as said below
- owner: int32 [64], replicated, may hold values from 0 to 7, as said below
Outputs:
- divergence: float32 [8, 32], P('grp')
- grad_student: bfloat16 [8, 32, 5120], P('grp', None, 'vocab')
The draws below stay inside these ranges and needn't reach their ends.
Inputs may be any that keep to these rules, and one draw needn't show every extreme that they name: All 8 sequences of one teacher group share one owner, and each student group owns the sequences of exactly one teacher group. The lengths of the 8 sequences of one teacher group sum to at most 32, and to exactly 32 for some group.
All inputs are finite; a program needn't handle non-finite values.
Results may differ from the reference program's by a relative error of at most 0.018.
Values may be sent and summed in bfloat16 or wider, within the bound.
A program may use at most 64 MiB of HBM per device.

```python
import jax
import jax.numpy as jnp
from jax import lax

DT = 4096
DS = 5120
VOC_DEV = 256
LMAX = 8
ROWS = 256
VOCAB = 8192
PAD = 32
SEQ_TEA = 8
SEQS = 64
N_GRP = 8
N_VOCAB = 4


def plan_groups(key):
    count = N_GRP
    seq_count = SEQ_TEA
    base_key = jax.random.fold_in(key, 7001)
    perm_key, level_key, star_key, unit_key = jax.random.split(base_key, 4)
    teacher_owner = jax.random.permutation(perm_key, count).astype(jnp.int32)
    owners = jnp.repeat(teacher_owner, seq_count)
    levels = jax.random.randint(level_key, (count,), 0, 65)
    totals = seq_count + (PAD - seq_count) * levels * levels // 4096
    starred = jax.random.randint(star_key, (), 0, count)
    marked_flag = jnp.arange(count) == starred
    totals = jnp.where(marked_flag, PAD, totals)
    extra = totals - seq_count
    unit_rows = LMAX - 1
    width = seq_count * unit_rows
    column_span = jnp.arange(width)
    score_values = jax.random.randint(unit_key, (count, width), 0, 1 << 16) * width + column_span[None, :]
    extra_reward = jnp.where(marked_flag[:, None] & (column_span[None, :] < unit_rows), 1 << 30, 0)
    score_values = score_values - extra_reward
    ranked = jnp.argsort(jnp.argsort(score_values, axis=1), axis=1)
    chosen = (ranked < extra[:, None]).astype(jnp.int32)
    seq_len = 1 + jnp.sum(chosen.reshape(count, seq_count, unit_rows), axis=2)
    return (owners.astype(jnp.int32), seq_len.reshape(-1).astype(jnp.int32))


def draw_lengths(key, part):
    return plan_groups(key)[1]


def draw_owner(key, part):
    return plan_groups(key)[0]


def hidden_values(key, shape):
    value_key = jax.random.fold_in(key, 0)
    values = jax.random.truncated_normal(value_key, -4.0, 4.0, shape, jnp.float32)
    return values


def draw_teacher_rows(key, part):
    return hidden_values(jax.random.fold_in(key, 311), (SEQS, LMAX, DT)).astype(jnp.bfloat16)


def draw_student_rows(key, part):
    return hidden_values(jax.random.fold_in(key, 523), (N_GRP, PAD, DS)).astype(jnp.bfloat16)


def block_scale(rng, extent, cuts, low, top_value):
    factor_of, own = 1.0, jax.random.fold_in(rng, 6)
    for position, blocks in cuts:
        draws = jnp.exp(jax.random.uniform(jax.random.fold_in(own, position), (blocks,), jnp.float32, low / len(cuts), top_value / len(cuts)))
        factor_of = factor_of * jnp.repeat(draws, extent[position] // blocks).reshape([-1 if axis == position else 1 for axis in range(len(extent))])
    return factor_of


def scatter_about(own_key, shape, scale, reach, cuts=(), kind=jnp.bfloat16):
    loudness = block_scale(own_key, shape, cuts, -0.22, 0.18) if cuts else 1.0
    values = jax.random.normal(own_key, shape, jnp.float32) * scale * loudness
    return jnp.minimum(jnp.maximum(values, -reach), reach).astype(kind)


def setup_inputs(seed: int = 0) -> dict:
    keys = jax.random.split(jax.random.key(seed), 7)
    return {
        "teacher_rows": draw_teacher_rows(jax.random.fold_in(keys[6], 71), 0),
        "student_rows": draw_student_rows(jax.random.fold_in(keys[6], 71), 0),
        "teacher_head": scatter_about(keys[2], (DT, VOCAB), (DT // 9) ** -0.5, 0.25, ((1, 32),)),
        "student_head": scatter_about(keys[3], (DS, VOCAB), (DS // 9) ** -0.5, 0.25, ((1, 32),)),
        "lengths": draw_lengths(jax.random.fold_in(keys[6], 71), 0),
        "owner": draw_owner(jax.random.fold_in(keys[6], 71), 0),
    }


def routing_tables(lengths, owner, groups, seq_count, positions, pad_rows):
    slot_count = seq_count * positions
    group_ids = jnp.arange(groups, dtype=jnp.int32)
    length_table = lengths.reshape(groups, seq_count)
    owner_table = owner.reshape(groups, seq_count)[:, 0]
    teacher_of = jnp.sum((owner_table[None, :] == group_ids[:, None]).astype(jnp.int32) * group_ids[None, :], axis=1).astype(jnp.int32)
    position_ids = jnp.arange(positions, dtype=jnp.int32)
    live_slots = (position_ids[None, None, :] < length_table[:, :, None]).reshape(groups, slot_count)
    ranked = jnp.cumsum(live_slots.astype(jnp.int32), axis=1) - 1
    target = jnp.where(live_slots, ranked, pad_rows).astype(jnp.int32)
    matches = target[:, None, :] == jnp.arange(pad_rows, dtype=jnp.int32)[None, :, None]
    source = jnp.sum(matches.astype(jnp.int32) * jnp.arange(slot_count, dtype=jnp.int32)[None, None, :], axis=2).astype(jnp.int32)
    totals = jnp.sum(length_table, axis=1).astype(jnp.int32)
    owned_total = jnp.take(totals, teacher_of, axis=0)
    student_live = jnp.arange(pad_rows, dtype=jnp.int32)[None, :] < owned_total[:, None]
    return teacher_of, source, student_live


def log_softmax_rows(logits):
    highest = jnp.max(logits, axis=-1, keepdims=True)
    shifted = logits - highest
    return shifted - jnp.log(jnp.sum(jnp.exp(shifted), axis=-1, keepdims=True))


def reference(teacher_rows, student_rows, teacher_head, student_head, lengths, owner):
    groups = N_GRP
    slot_count = SEQ_TEA * LMAX
    teacher_of, source, student_live = routing_tables(lengths, owner, groups, SEQ_TEA, LMAX, PAD)
    row_position = (teacher_of[:, None] * slot_count + jnp.take(source, teacher_of, axis=0)).reshape(ROWS).astype(jnp.int32)
    arrived = jnp.take(teacher_rows.reshape(groups * slot_count, DT), row_position, axis=0)
    student_block = student_rows.reshape(ROWS, DS)
    teacher_logits = jnp.dot(arrived, teacher_head, preferred_element_type=jnp.float32)
    student_logits = jnp.dot(student_block, student_head, preferred_element_type=jnp.float32)
    log_p = log_softmax_rows(teacher_logits)
    log_q = log_softmax_rows(student_logits)
    student_prob = jnp.exp(log_q)
    log_ratio = log_q - log_p
    weight = student_live.reshape(ROWS).astype(jnp.float32)
    kl_rows = jnp.sum(student_prob * log_ratio, axis=-1) * weight
    grad_logits = (weight[:, None] * student_prob * (log_ratio - kl_rows[:, None])).astype(jnp.bfloat16)

    def add_block(shard, running):
        offset = (shard * VOC_DEV).astype(jnp.int32)
        grad_block = lax.dynamic_slice_in_dim(grad_logits, offset, VOC_DEV, 1)
        head_block = lax.dynamic_slice_in_dim(student_head, offset, VOC_DEV, 1)
        partial_value = jnp.dot(grad_block, head_block.T, preferred_element_type=jnp.float32)
        rounded = lax.optimization_barrier(partial_value.astype(jnp.bfloat16))
        return running + rounded.astype(jnp.float32)

    summed = lax.fori_loop(0, N_GRP * N_VOCAB, add_block, jnp.zeros((ROWS, DS), jnp.float32))
    divergence = kl_rows.reshape(groups, PAD)
    grad_student = summed.astype(jnp.bfloat16).reshape(groups, PAD, DS)
    return divergence, grad_student
```

```python
import functools

import jax
import jax.numpy as jnp
from jax import lax
from jax.experimental import pallas as pl
from jax.experimental.pallas import tpu as pltpu
from jax.sharding import PartitionSpec as P

MESH = pl.DeviceIdType.MESH
PIECES = 8
f32 = jnp.float32


def place():
    g, v = lax.axis_index("grp"), lax.axis_index("vocab")
    return g, v, v // 2, lax.rem(v, 2)


def enter(g, v, peers):
    barrier = pltpu.get_barrier_semaphore()
    for peer in peers:
        pl.semaphore_signal(barrier, inc=1, device_id=peer, device_id_type=MESH)
    pl.semaphore_wait(barrier, len(peers))


def tree_peers(g, v, y, c, groups, lines):
    peers = [(g, v + 1 - 2 * c)]
    peers += [(g, lax.rem(y + j, lines) * 2 + c) for j in range(1, lines)]
    peers += [(lax.rem(g + k, groups), v) for k in range(1, groups)]
    return peers


def send(src, dst, send_sem, recv_sem, device):
    return pltpu.make_async_remote_copy(
        src_ref=src, dst_ref=dst, send_sem=send_sem, recv_sem=recv_sem,
        device_id=device, device_id_type=MESH,
    )


def gather_kernel(groups, lines, pieces, t_in, s_in, t_out, s_out, gs, gr, ys, yr, cs, cr):
    g, v, y, c = place()
    per = groups // pieces
    pairs = ((t_in, t_out), (s_in, s_out))
    for src, out in pairs:
        out[v, g] = src[...]
    enter(g, v, tree_peers(g, v, y, c, groups, lines))
    first = g // per
    across = (g, v + 1 - 2 * c)
    waits = []

    def grp_copy(a, k):
        src, out = pairs[a]
        return send(src, out.at[v, g], gs.at[a, k], gr.at[a, k], (lax.rem(g + k, groups), v))

    def line_copy(a, j, kp):
        out = pairs[a][1]
        piece = out.at[v, pl.ds(lax.rem(first - kp + pieces, pieces) * per, per)]
        return send(piece, piece, ys.at[a, j, kp], yr.at[a, j, kp],
                    (g, lax.rem(y + j, lines) * 2 + c))

    def core_copy(a, j):
        out = pairs[a][1]
        slot = out.at[lax.rem(y - j + lines, lines) * 2 + c]
        return send(slot, slot, cs.at[a, j], cr.at[a, j], across)

    for k in range(1, groups):
        for a in range(2):
            copy = grp_copy(a, k)
            copy.start()
            waits.append(copy)
    for kp in range(pieces):
        for a in range(2):
            for i in range(per):
                block = lax.rem(first - kp + pieces, pieces) * per + i
                k = lax.rem(g - block + groups, groups)

                if per == 1:
                    if kp > 0:
                        grp_copy(a, kp).wait_recv()
                else:
                    @pl.when(k > 0)
                    def _():
                        send(pairs[a][0], pairs[a][1].at[v, g], gs.at[a, k], gr.at[a, k],
                             across).wait_recv()
            for j in range(1, lines):
                copy = line_copy(a, j, kp)
                copy.start()
                waits.append(copy)
    for a in range(2):
        copy = core_copy(a, 0)
        copy.start()
        waits.append(copy)
    for j in range(1, lines):
        for a in range(2):
            for kp in range(pieces):
                line_copy(a, j, kp).wait_recv()
            copy = core_copy(a, j)
            copy.start()
            waits.append(copy)
    for j in range(lines):
        for a in range(2):
            core_copy(a, j).wait_recv()
    for copy in waits:
        copy.wait_send()


def stats_kernel(groups, width, mine, out, gs, gr, vs, vr):
    g, v, _, _ = place()
    out[v, g] = mine[...]
    peers = [(g, lax.rem(v + j, width)) for j in range(1, width)]
    peers += [(lax.rem(g + k, groups), v) for k in range(1, groups)]
    enter(g, v, peers)
    near = [
        send(mine, out.at[v, g], gs.at[k], gr.at[k], (lax.rem(g + k, groups), v))
        for k in range(1, groups)
    ]
    for copy in near:
        copy.start()
    for copy in near:
        copy.wait_recv()
    wide = [
        send(out.at[v], out.at[v], vs.at[j], vr.at[j], (g, lax.rem(v + j, width)))
        for j in range(1, width)
    ]
    for copy in wide:
        copy.start()
    for copy in wide:
        copy.wait_recv()
    for copy in near + wide:
        copy.wait_send()


def scatter_kernel(groups, lines, pieces, part, out, cbuf, ysum, ybuf, gsum, gbuf, acc,
                   cs, cr, ys, yr, gs, gr):
    g, v, y, c = place()
    per = groups // pieces
    first = g // per
    enter(g, v, tree_peers(g, v, y, c, groups, lines))
    other = 1 - c

    def line_of(j):
        return lax.rem(y + j, lines)

    core = [
        send(part.at[line_of(j) * 2 + other], cbuf.at[j], cs.at[j], cr.at[j], (g, v + 1 - 2 * c))
        for j in range(lines)
    ]
    for j in list(range(1, lines)) + [0]:
        core[j].start()
    waits = list(core)
    order = list(range(1, pieces)) + [0]
    line = {}
    for j in range(1, lines):
        core[j].wait_recv()
        for kp in order:
            low = lax.rem(first + kp, pieces) * per
            span = pl.ds(low, per)
            ysum[j, span] = (
                part[line_of(j) * 2 + c, span].astype(f32) + cbuf[j, span].astype(f32)
            ).astype(jnp.bfloat16)
            copy = send(ysum.at[j, span], ybuf.at[j, span], ys.at[j, kp], yr.at[j, kp],
                        (g, line_of(j) * 2 + c))
            copy.start()
            line[j, kp] = copy
            waits.append(copy)
    core[0].wait_recv()

    def total(block):
        value = part[v, block].astype(f32) + cbuf[0, block].astype(f32)
        for j in range(1, lines):
            value = value + ybuf[j, block].astype(f32)
        return value

    def far(k, device):
        return send(gsum.at[k], gbuf.at[k], gs.at[k], gr.at[k], device)

    for kp in order:
        for j in range(1, lines):
            line[j, kp].wait_recv()
        for i in range(per):
            block = lax.rem(first + kp, pieces) * per + i
            k = lax.rem(block - g + groups, groups)
            if per == 1:
                if kp == 0:
                    acc[...] = total(g)
                else:
                    gsum[kp] = total(block).astype(jnp.bfloat16)
                    far(kp, (block, v)).start()
            else:
                @pl.when(k == 0)
                def _():
                    acc[...] = total(block)

                @pl.when(k > 0)
                def _():
                    gsum[k] = total(block).astype(jnp.bfloat16)
                    far(k, (block, v)).start()
    value = acc[...]
    for k in range(1, groups):
        far(k, (lax.rem(g + k, groups), v)).wait_recv()
        value = value + gbuf[k].astype(f32)
    out[...] = value.astype(jnp.bfloat16)
    for copy in waits:
        copy.wait_send()
    for k in range(1, groups):
        far(k, (lax.rem(g + k, groups), v)).wait_send()


VM = pl.BlockSpec(memory_space=pltpu.VMEM)
DMA = pltpu.SemaphoreType.DMA


def params(number):
    return pltpu.CompilerParams(
        collective_id=number, has_side_effects=True, vmem_limit_bytes=48 * 1024 * 1024
    )


def per_device(teacher_rows, student_rows, teacher_head, student_head, lengths, owner):
    groups, width = lax.axis_size("grp"), lax.axis_size("vocab")
    lines = width // 2
    pieces = PIECES if groups % PIECES == 0 else groups
    seqs, positions, dt = teacher_rows.shape
    _, pad, ds = student_rows.shape
    slots, rows, vocab = seqs * positions, groups * pad, teacher_head.shape[1]
    own = lax.axis_index("grp")
    ids = jnp.arange(groups, dtype=jnp.int32)
    table = lengths.reshape(groups, seqs)
    owned = owner.reshape(groups, seqs)[:, 0][None, :] == ids[:, None]
    totals = jnp.sum(table, axis=1)
    live = jnp.arange(pad, dtype=jnp.int32)[None, :] < jnp.sum(
        jnp.where(owned, totals[None, :], 0), axis=1
    )[:, None]
    mine = lax.dynamic_index_in_dim(table, own, 0, keepdims=False)
    seq_ids = jnp.arange(seqs, dtype=jnp.int32)
    starts = jnp.sum(jnp.where(seq_ids[None, :] < seq_ids[:, None], mine[None, :], 0), axis=1)
    pos = jnp.arange(positions, dtype=jnp.int32)
    target = jnp.where(pos[None, :] < mine[:, None], starts[:, None] + pos[None, :], -1)
    target = target.reshape(slots)
    k_ids = jnp.arange(pad, dtype=jnp.int32)
    pick = (target[None, :] == k_ids[:, None]) | (
        (k_ids[:, None] >= jnp.sum(mine)) & (jnp.arange(slots)[None, :] == 0)
    )
    sent = jnp.dot(
        pick.astype(jnp.bfloat16), teacher_rows.reshape(slots, dt), preferred_element_type=f32
    ).astype(jnp.bfloat16)

    t_all, s_all = pl.pallas_call(
        functools.partial(gather_kernel, groups, lines, pieces),
        out_shape=(
            jax.ShapeDtypeStruct((width, groups, pad, dt), jnp.bfloat16),
            jax.ShapeDtypeStruct((width, groups, pad, ds), jnp.bfloat16),
        ),
        in_specs=[VM, VM],
        out_specs=(VM, VM),
        scratch_shapes=[
            DMA((2, groups)), DMA((2, groups)),
            DMA((2, lines, pieces)), DMA((2, lines, pieces)),
            DMA((2, lines)), DMA((2, lines)),
        ],
        compiler_params=params(0),
    )(sent, student_rows.reshape(pad, ds))

    raw = jnp.einsum(
        "vrd,vdn->rn", t_all.reshape(width, rows, dt), teacher_head.reshape(width, dt, vocab),
        preferred_element_type=f32,
    ).reshape(groups, pad, vocab)
    head = student_head.reshape(width, ds, vocab)
    s = jnp.einsum("vrd,vdn->rn", s_all.reshape(width, rows, ds), head, preferred_element_type=f32)
    t = jnp.sum(jnp.where(owned[:, :, None, None], raw[None], 0.0), axis=1).reshape(rows, vocab)

    t_top, s_top = jnp.max(t, axis=1), jnp.max(s, axis=1)
    s_exp = jnp.exp(s - s_top[:, None])
    zero = jnp.zeros((rows,), f32)
    stats = jnp.stack([
        t_top, jnp.sum(jnp.exp(t - t_top[:, None]), axis=1),
        s_top, jnp.sum(s_exp, axis=1), jnp.sum(s_exp * (s - t), axis=1), zero, zero, zero,
    ])
    every = pl.pallas_call(
        functools.partial(stats_kernel, groups, width),
        out_shape=jax.ShapeDtypeStruct((width, groups, 8, rows), f32),
        in_specs=[VM],
        out_specs=VM,
        scratch_shapes=[DMA((groups,)), DMA((groups,)), DMA((width,)), DMA((width,))],
        compiler_params=params(1),
    )(stats).reshape(width * groups, 8, rows)
    t_max, s_max = jnp.max(every[:, 0], axis=0), jnp.max(every[:, 2], axis=0)
    s_scale = jnp.exp(every[:, 2] - s_max)
    t_lse = t_max + jnp.log(jnp.sum(every[:, 1] * jnp.exp(every[:, 0] - t_max), axis=0))
    s_total = jnp.sum(every[:, 3] * s_scale, axis=0)
    s_lse = s_max + jnp.log(s_total)
    cross = jnp.sum(every[:, 4] * s_scale, axis=0) / s_total
    weight = live.reshape(-1).astype(f32)
    kl = (cross - (s_lse - t_lse)) * weight
    log_q = s - s_lse[:, None]
    log_p = t - t_lse[:, None]
    grad = (weight[:, None] * jnp.exp(log_q) * (log_q - log_p - kl[:, None])).astype(jnp.bfloat16)
    part = jnp.einsum("rn,vdn->vrd", grad, head, preferred_element_type=f32).astype(jnp.bfloat16)
    block = (groups, pad, ds)
    out = pl.pallas_call(
        functools.partial(scatter_kernel, groups, lines, pieces),
        out_shape=jax.ShapeDtypeStruct((pad, ds), jnp.bfloat16),
        in_specs=[VM],
        out_specs=VM,
        scratch_shapes=[
            pltpu.VMEM((lines,) + block, jnp.bfloat16),
            pltpu.VMEM((lines,) + block, jnp.bfloat16),
            pltpu.VMEM((lines,) + block, jnp.bfloat16),
            pltpu.VMEM(block, jnp.bfloat16),
            pltpu.VMEM(block, jnp.bfloat16),
            pltpu.VMEM((pad, ds), f32),
            DMA((lines,)), DMA((lines,)),
            DMA((lines, pieces)), DMA((lines, pieces)),
            DMA((groups,)), DMA((groups,)),
        ],
        compiler_params=params(2),
    )(part.reshape((width,) + block))
    divergence = lax.dynamic_slice_in_dim(kl, own * pad, pad, 0)
    return divergence.reshape(1, pad), out.reshape(1, pad, ds)


def solution(mesh):
    placed = (
        P("grp", None, "vocab"),
        P("grp", None, "vocab"),
        P(None, ("grp", "vocab")),
        P(None, ("grp", "vocab")),
        P(),
        P(),
    )
    return jax.shard_map(
        per_device,
        mesh=mesh,
        in_specs=placed,
        out_specs=(P("grp", None), P("grp", None, "vocab")),
        check_vma=False,
    )
```

```python
import functools

import jax
import jax.numpy as jnp
from jax import lax
from jax.experimental import pallas as pl
from jax.experimental.pallas import tpu as pltpu
from jax.sharding import PartitionSpec as P

MESH = pl.DeviceIdType.MESH
PIECES = 8
f32 = jnp.float32


def place():
    g, v = lax.axis_index("grp"), lax.axis_index("vocab")
    return g, v, v // 2, lax.rem(v, 2)


def enter(g, v, peers):
    barrier = pltpu.get_barrier_semaphore()
    for peer in peers:
        pl.semaphore_signal(barrier, inc=1, device_id=peer, device_id_type=MESH)
    pl.semaphore_wait(barrier, len(peers))


def tree_peers(g, v, y, c, groups, lines):
    peers = [(g, v + 1 - 2 * c)]
    peers += [(g, lax.rem(y + j, lines) * 2 + c) for j in range(1, lines)]
    peers += [(lax.rem(g + k, groups), v) for k in range(1, groups)]
    return peers


def send(src, dst, send_sem, recv_sem, device):
    return pltpu.make_async_remote_copy(
        src_ref=src, dst_ref=dst, send_sem=send_sem, recv_sem=recv_sem,
        device_id=device, device_id_type=MESH,
    )


def gather_kernel(groups, lines, pieces, t_in, s_in, t_out, s_out, gs, gr, ys, yr, cs, cr):
    g, v, y, c = place()
    per = groups // pieces
    pairs = ((t_in, t_out), (s_in, s_out))
    for src, out in pairs:
        out[v, g] = src[...]
    enter(g, v, tree_peers(g, v, y, c, groups, lines))
    first = g // per
    across = (g, v + 1 - 2 * c)
    waits = []

    def grp_copy(a, k):
        src, out = pairs[a]
        return send(src, out.at[v, g], gs.at[a, k], gr.at[a, k], (lax.rem(g + k, groups), v))

    def line_copy(a, j, kp):
        out = pairs[a][1]
        piece = out.at[v, pl.ds(lax.rem(first - kp + pieces, pieces) * per, per)]
        return send(piece, piece, ys.at[a, j, kp], yr.at[a, j, kp],
                    (g, lax.rem(y + j, lines) * 2 + c))

    def core_copy(a, j, kp):
        out = pairs[a][1]
        slot = out.at[lax.rem(y - j + lines, lines) * 2 + c,
                      pl.ds(lax.rem(first - kp + pieces, pieces) * per, per)]
        return send(slot, slot, cs.at[a, j, kp], cr.at[a, j, kp], across)

    for k in range(1, groups):
        for a in range(2):
            copy = grp_copy(a, k)
            copy.start()
            waits.append(copy)
    for kp in range(pieces):
        for a in range(2):
            for i in range(per):
                block = lax.rem(first - kp + pieces, pieces) * per + i
                k = lax.rem(g - block + groups, groups)

                if per == 1:
                    if kp > 0:
                        grp_copy(a, kp).wait_recv()
                else:
                    @pl.when(k > 0)
                    def _():
                        send(pairs[a][0], pairs[a][1].at[v, g], gs.at[a, k], gr.at[a, k],
                             across).wait_recv()
            for j in range(1, lines):
                copy = line_copy(a, j, kp)
                copy.start()
                waits.append(copy)
            copy = core_copy(a, 0, kp)
            copy.start()
            waits.append(copy)
    for j in range(1, lines):
        for kp in range(pieces):
            for a in range(2):
                line_copy(a, j, kp).wait_recv()
                copy = core_copy(a, j, kp)
                copy.start()
                waits.append(copy)
    for j in range(lines):
        for kp in range(pieces):
            for a in range(2):
                core_copy(a, j, kp).wait_recv()
    for copy in waits:
        copy.wait_send()


def stats_kernel(groups, width, mine, out, gs, gr, vs, vr):
    g, v, _, _ = place()
    out[v, g] = mine[...]
    peers = [(g, lax.rem(v + j, width)) for j in range(1, width)]
    peers += [(lax.rem(g + k, groups), v) for k in range(1, groups)]
    enter(g, v, peers)
    near = [
        send(mine, out.at[v, g], gs.at[k], gr.at[k], (lax.rem(g + k, groups), v))
        for k in range(1, groups)
    ]
    for copy in near:
        copy.start()
    for copy in near:
        copy.wait_recv()
    wide = [
        send(out.at[v], out.at[v], vs.at[j], vr.at[j], (g, lax.rem(v + j, width)))
        for j in range(1, width)
    ]
    for copy in wide:
        copy.start()
    for copy in wide:
        copy.wait_recv()
    for copy in near + wide:
        copy.wait_send()


def scatter_kernel(groups, lines, pieces, part, out, cbuf, ysum, ybuf, gsum, gbuf, acc,
                   cs, cr, ys, yr, gs, gr):
    g, v, y, c = place()
    per = groups // pieces
    first = g // per
    enter(g, v, tree_peers(g, v, y, c, groups, lines))
    other = 1 - c

    def line_of(j):
        return lax.rem(y + j, lines)

    core = [
        send(part.at[line_of(j) * 2 + other], cbuf.at[j], cs.at[j], cr.at[j], (g, v + 1 - 2 * c))
        for j in range(lines)
    ]
    for j in list(range(1, lines)) + [0]:
        core[j].start()
    waits = list(core)
    order = list(range(1, pieces)) + [0]
    line = {}
    for j in range(1, lines):
        core[j].wait_recv()
        for kp in order:
            low = lax.rem(first + kp, pieces) * per
            span = pl.ds(low, per)
            ysum[j, span] = (
                part[line_of(j) * 2 + c, span].astype(f32) + cbuf[j, span].astype(f32)
            ).astype(jnp.bfloat16)
            copy = send(ysum.at[j, span], ybuf.at[j, span], ys.at[j, kp], yr.at[j, kp],
                        (g, line_of(j) * 2 + c))
            copy.start()
            line[j, kp] = copy
            waits.append(copy)
    core[0].wait_recv()

    def total(block):
        value = part[v, block].astype(f32) + cbuf[0, block].astype(f32)
        for j in range(1, lines):
            value = value + ybuf[j, block].astype(f32)
        return value

    def far(k, device):
        return send(gsum.at[k], gbuf.at[k], gs.at[k], gr.at[k], device)

    for kp in order:
        for j in range(1, lines):
            line[j, kp].wait_recv()
        for i in range(per):
            block = lax.rem(first + kp, pieces) * per + i
            k = lax.rem(block - g + groups, groups)
            if per == 1:
                if kp == 0:
                    acc[...] = total(g)
                else:
                    gsum[kp] = total(block).astype(jnp.bfloat16)
                    far(kp, (block, v)).start()
            else:
                @pl.when(k == 0)
                def _():
                    acc[...] = total(block)

                @pl.when(k > 0)
                def _():
                    gsum[k] = total(block).astype(jnp.bfloat16)
                    far(k, (block, v)).start()
    value = acc[...]
    for k in range(1, groups):
        far(k, (lax.rem(g + k, groups), v)).wait_recv()
        value = value + gbuf[k].astype(f32)
    out[...] = value.astype(jnp.bfloat16)
    for copy in waits:
        copy.wait_send()
    for k in range(1, groups):
        far(k, (lax.rem(g + k, groups), v)).wait_send()


VM = pl.BlockSpec(memory_space=pltpu.VMEM)
DMA = pltpu.SemaphoreType.DMA


def params(number):
    return pltpu.CompilerParams(
        collective_id=number, has_side_effects=True, vmem_limit_bytes=48 * 1024 * 1024
    )


def per_device(teacher_rows, student_rows, teacher_head, student_head, lengths, owner):
    groups, width = lax.axis_size("grp"), lax.axis_size("vocab")
    lines = width // 2
    pieces = PIECES if groups % PIECES == 0 else groups
    seqs, positions, dt = teacher_rows.shape
    _, pad, ds = student_rows.shape
    slots, rows, vocab = seqs * positions, groups * pad, teacher_head.shape[1]
    own = lax.axis_index("grp")
    ids = jnp.arange(groups, dtype=jnp.int32)
    table = lengths.reshape(groups, seqs)
    owned = owner.reshape(groups, seqs)[:, 0][None, :] == ids[:, None]
    totals = jnp.sum(table, axis=1)
    live = jnp.arange(pad, dtype=jnp.int32)[None, :] < jnp.sum(
        jnp.where(owned, totals[None, :], 0), axis=1
    )[:, None]
    mine = lax.dynamic_index_in_dim(table, own, 0, keepdims=False)
    seq_ids = jnp.arange(seqs, dtype=jnp.int32)
    starts = jnp.sum(jnp.where(seq_ids[None, :] < seq_ids[:, None], mine[None, :], 0), axis=1)
    pos = jnp.arange(positions, dtype=jnp.int32)
    target = jnp.where(pos[None, :] < mine[:, None], starts[:, None] + pos[None, :], -1)
    target = target.reshape(slots)
    k_ids = jnp.arange(pad, dtype=jnp.int32)
    pick = (target[None, :] == k_ids[:, None]) | (
        (k_ids[:, None] >= jnp.sum(mine)) & (jnp.arange(slots)[None, :] == 0)
    )
    sent = jnp.dot(
        pick.astype(jnp.bfloat16), teacher_rows.reshape(slots, dt), preferred_element_type=f32
    ).astype(jnp.bfloat16)

    t_all, s_all = pl.pallas_call(
        functools.partial(gather_kernel, groups, lines, pieces),
        out_shape=(
            jax.ShapeDtypeStruct((width, groups, pad, dt), jnp.bfloat16),
            jax.ShapeDtypeStruct((width, groups, pad, ds), jnp.bfloat16),
        ),
        in_specs=[VM, VM],
        out_specs=(VM, VM),
        scratch_shapes=[
            DMA((2, groups)), DMA((2, groups)),
            DMA((2, lines, pieces)), DMA((2, lines, pieces)),
            DMA((2, lines, pieces)), DMA((2, lines, pieces)),
        ],
        compiler_params=params(0),
    )(sent, student_rows.reshape(pad, ds))

    raw = jnp.einsum(
        "vrd,vdn->rn", t_all.reshape(width, rows, dt), teacher_head.reshape(width, dt, vocab),
        preferred_element_type=f32,
    ).reshape(groups, pad, vocab)
    head = student_head.reshape(width, ds, vocab)
    s = jnp.einsum("vrd,vdn->rn", s_all.reshape(width, rows, ds), head, preferred_element_type=f32)
    t = jnp.sum(jnp.where(owned[:, :, None, None], raw[None], 0.0), axis=1).reshape(rows, vocab)

    t_top, s_top = jnp.max(t, axis=1), jnp.max(s, axis=1)
    s_exp = jnp.exp(s - s_top[:, None])
    zero = jnp.zeros((rows,), f32)
    stats = jnp.stack([
        t_top, jnp.sum(jnp.exp(t - t_top[:, None]), axis=1),
        s_top, jnp.sum(s_exp, axis=1), jnp.sum(s_exp * (s - t), axis=1), zero, zero, zero,
    ])
    every = pl.pallas_call(
        functools.partial(stats_kernel, groups, width),
        out_shape=jax.ShapeDtypeStruct((width, groups, 8, rows), f32),
        in_specs=[VM],
        out_specs=VM,
        scratch_shapes=[DMA((groups,)), DMA((groups,)), DMA((width,)), DMA((width,))],
        compiler_params=params(1),
    )(stats).reshape(width * groups, 8, rows)
    t_max, s_max = jnp.max(every[:, 0], axis=0), jnp.max(every[:, 2], axis=0)
    s_scale = jnp.exp(every[:, 2] - s_max)
    t_lse = t_max + jnp.log(jnp.sum(every[:, 1] * jnp.exp(every[:, 0] - t_max), axis=0))
    s_total = jnp.sum(every[:, 3] * s_scale, axis=0)
    s_lse = s_max + jnp.log(s_total)
    cross = jnp.sum(every[:, 4] * s_scale, axis=0) / s_total
    weight = live.reshape(-1).astype(f32)
    kl = (cross - (s_lse - t_lse)) * weight
    log_q = s - s_lse[:, None]
    log_p = t - t_lse[:, None]
    grad = (weight[:, None] * jnp.exp(log_q) * (log_q - log_p - kl[:, None])).astype(jnp.bfloat16)
    part = jnp.einsum("rn,vdn->vrd", grad, head, preferred_element_type=f32).astype(jnp.bfloat16)
    block = (groups, pad, ds)
    out = pl.pallas_call(
        functools.partial(scatter_kernel, groups, lines, pieces),
        out_shape=jax.ShapeDtypeStruct((pad, ds), jnp.bfloat16),
        in_specs=[VM],
        out_specs=VM,
        scratch_shapes=[
            pltpu.VMEM((lines,) + block, jnp.bfloat16),
            pltpu.VMEM((lines,) + block, jnp.bfloat16),
            pltpu.VMEM((lines,) + block, jnp.bfloat16),
            pltpu.VMEM(block, jnp.bfloat16),
            pltpu.VMEM(block, jnp.bfloat16),
            pltpu.VMEM((pad, ds), f32),
            DMA((lines,)), DMA((lines,)),
            DMA((lines, pieces)), DMA((lines, pieces)),
            DMA((groups,)), DMA((groups,)),
        ],
        compiler_params=params(2),
    )(part.reshape((width,) + block))
    divergence = lax.dynamic_slice_in_dim(kl, own * pad, pad, 0)
    return divergence.reshape(1, pad), out.reshape(1, pad, ds)


def solution(mesh):
    placed = (
        P("grp", None, "vocab"),
        P("grp", None, "vocab"),
        P(None, ("grp", "vocab")),
        P(None, ("grp", "vocab")),
        P(),
        P(),
    )
    return jax.shard_map(
        per_device,
        mesh=mesh,
        in_specs=placed,
        out_specs=(P("grp", None), P("grp", None, "vocab")),
        check_vma=False,
    )
```
